32 devices in a mesh: rep: 1, samp: 32 (over z, y, x, core), snp: 1.
Axes of the slice: x: 2, y: 2, z: 4, core: 2. Of those that a mesh axis runs over, the one named last changes fastest.
Arguments:
- genotypes: bfloat16 [6144, 65536], P('samp', 'snp'), may hold values from -4 to 4
- counts: int32 [6144], P(('rep', 'samp')), may hold values from 0 to 3
- phenotypes: float32 [8, 6144], P(None, 'samp'), may hold values from -12 to 12
Outputs:
- solution: float32 [8, 6144], P(None, ('rep', 'samp'))
- residual: float32 [8, 6144], P(None, ('rep', 'samp'))
The draws below stay inside these ranges and needn't reach their ends.
All inputs are finite; a program needn't handle non-finite values.
Results may differ from the reference program's by a relative error of at most 0.012.
The reference program's roundings to bfloat16 on the way count: a program that leaves them out, or rounds other values in their place, can miss the bound.
Values may be sent and summed in bfloat16 or wider, within the bound.
No kernel may reach another device: no remote copies, remote signals or barrier semaphores. Data moves between devices by JAX's collectives and lax.ppermute only.
A program may use at most 64 MiB of HBM per device.

```python
import jax
import jax.numpy as jnp
from jax import lax

SNPS = 65536
RHS = 8
ITERS = 2
SAMPLES = 6144


def draw_phenotypes(key, part):
    first = jax.random.fold_in(key, 11)
    place = jnp.arange(SAMPLES, dtype=jnp.float32)[None, :] / SAMPLES
    values = jnp.clip(jax.random.normal(first, (RHS, SAMPLES), jnp.float32), -4.0, 4.0)
    return 0.3 * 10.0 ** place * values


def plant(entries, rng, least, largest):
    shape = entries.shape
    index_at = [jax.random.randint(jax.random.fold_in(rng, axis), (), 0, shape[axis]) for axis in range(len(shape))]
    entries = entries.at[tuple(index_at)].set(least)
    longest = shape.index(max(shape))
    index_at[longest] = (index_at[longest] + 1) % shape[longest]
    return entries.at[tuple(index_at)].set(largest)


def block_scale(own_key, dims, split, smallest, high):
    level = 1.0
    for axis_at, shards_of in split:
        heights = jax.random.uniform(jax.random.fold_in(jax.random.fold_in(own_key, 6), axis_at), (shards_of,), jnp.float32, smallest / len(split), high / len(split))
        level = level * jnp.repeat(jnp.exp(heights), dims[axis_at] // shards_of).reshape((-1,) + (1,) * (len(dims) - 1 - axis_at))
    return level


def noise(key, dims, scale, most, pieces=(), kind=jnp.bfloat16):
    gain = block_scale(key, dims, pieces, -0.22, 0.18) if pieces else 1.0
    drawn = jax.random.normal(key, dims, jnp.float32) * scale * gain
    return jnp.minimum(jnp.maximum(drawn, -most), most).astype(kind)


def setup_inputs(seed: int = 0, part: int = 0) -> dict:
    key_of = jax.random.split(jax.random.key(seed), 4)
    own_keys = jax.random.split(jax.random.fold_in(key_of[3], part), 4)
    genotypes = noise(key_of[0], (SAMPLES, SNPS), 1.0, 4.0, ((0, 32),))
    counts = plant(jax.random.randint(own_keys[1], (SAMPLES,), 0, 4), jax.random.fold_in(own_keys[1], 1), 0, 3).astype(jnp.int32)
    phenotypes = draw_phenotypes(jax.random.fold_in(key_of[3], 71), part)
    return {"genotypes": genotypes, "counts": counts, "phenotypes": phenotypes}


ridge = 1.0

def operate(block, root, genotypes):
    weighted = (root[None, :] * block).astype(jnp.bfloat16)
    per_snp = jnp.dot(weighted, genotypes, preferred_element_type=jnp.float32).astype(jnp.bfloat16)
    back = lax.dot_general(per_snp, genotypes, (((1,), (1,)), ((), ())), preferred_element_type=jnp.float32)
    return root[None, :] * back / SNPS + ridge * block

def reference(genotypes, counts, phenotypes):
    root = jnp.sqrt(counts.astype(jnp.float32))
    solution = jnp.zeros_like(phenotypes)
    residual = phenotypes
    direction = phenotypes
    norm_now = lax.optimization_barrier(jnp.sum(residual * residual, axis=1))
    for step in range(ITERS):
        image = operate(direction, root, genotypes)
        alpha = norm_now / lax.optimization_barrier(jnp.sum(direction * image, axis=1))
        solution = solution + alpha[:, None] * direction
        residual = residual - alpha[:, None] * image
        norm_next = lax.optimization_barrier(jnp.sum(residual * residual, axis=1))
        direction = residual + (norm_next / norm_now)[:, None] * direction
        norm_now = norm_next
    return (solution, residual)
```

```python
import jax
import jax.numpy as jnp
from jax import lax
from jax.experimental import pallas as pl
from jax.experimental.pallas import tpu as pltpu
from jax.sharding import PartitionSpec as P

ridge = 1.0
CHUNKS = 2
LANES = 128


def first_pass_kernel(pieces, width):
    half = pieces // 2

    def body(place_ref, q_ref, g_ref, send_ref, keep_ref, held_ref, sems):
        def copy_of(p):
            at = pl.multiple_of((place_ref[0] + (p ^ place_ref[1])) * width, width)
            return pltpu.make_async_copy(
                g_ref.at[:, pl.ds(at, width)], held_ref.at[:, pl.ds(p * width, width)], sems.at[p]
            )

        order = list(range(half, pieces)) + list(range(half))
        for p in order:
            copy_of(p).start()
        q = q_ref[...]
        for p in order:
            copy_of(p).wait()
            sums = jnp.dot(q, held_ref[:, p * width : (p + 1) * width], preferred_element_type=jnp.float32)
            if p >= half:
                send_ref[:, (p - half) * width : (p - half + 1) * width] = sums.astype(jnp.bfloat16)
            else:
                keep_ref[:, p * width : (p + 1) * width] = sums

    return body


def pass_kernel(pieces, width):
    half = pieces // 2

    def body(q_ref, held_ref, send_ref, keep_ref):
        q = q_ref[...]
        for p in list(range(half, pieces)) + list(range(half)):
            sums = jnp.dot(q, held_ref[:, p * width : (p + 1) * width], preferred_element_type=jnp.float32)
            if p >= half:
                send_ref[:, (p - half) * width : (p - half + 1) * width] = sums.astype(jnp.bfloat16)
            else:
                keep_ref[:, p * width : (p + 1) * width] = sums

    return body


def back_kernel(widths, step):
    def body(*refs):
        part_refs = refs[: len(widths)]
        held_ref, back_ref, square_ref = refs[len(widths) :]
        back = jnp.zeros(back_ref.shape, jnp.float32)
        square = jnp.zeros(square_ref.shape, jnp.float32)
        base = 0
        for part_ref, width in zip(part_refs, widths):
            for at in range(0, width, step):
                t = part_ref[:, at : at + step]
                back = back + lax.dot_general(
                    held_ref[:, base + at : base + at + step],
                    t,
                    (((1,), (1,)), ((), ())),
                    preferred_element_type=jnp.float32,
                )
                wide = t.astype(jnp.float32)
                wide = wide * wide
                for lane in range(0, step, LANES):
                    square = square + wide[:, lane : lane + LANES]
            base += width
        back_ref[...] = back
        square_ref[...] = square

    return body


def vmem():
    return pl.BlockSpec(memory_space=pltpu.VMEM)


def smem():
    return pl.BlockSpec(memory_space=pltpu.SMEM)


def params():
    return pltpu.CompilerParams(vmem_limit_bytes=24 * 2**20)


def rounded(x):
    return lax.reduce_precision(x, 8, 7)


def split3(x):
    high = rounded(x)
    middle = rounded(x - high)
    low = rounded(x - high - middle)
    lane = lax.broadcasted_iota(jnp.int32, (x.shape[0], LANES), 1)
    out = jnp.where(lane == 0, high[:, None], jnp.where(lane == 1, middle[:, None], jnp.where(lane == 2, low[:, None], 0.0)))
    return out.astype(jnp.bfloat16)


def join3(x):
    return jnp.sum(x.astype(jnp.float32), axis=1)


def solution(mesh):
    ranks = mesh.shape["samp"]
    snp_ranks = mesh.shape["snp"]
    bits = ranks.bit_length() - 1
    assert ranks == 1 << bits and bits >= 4
    levels = 3
    pieces = 1 << levels
    full_masks = [1 << b for b in range(levels, bits - 1)] + [(1 << (bits - 1)) | (1 << (bits - 2))]
    if bits - levels == 1:
        full_masks = [1 << (bits - 1)]
    halving = [[1, 2, 4], [1, 4, 2]]

    def swap(x, mask):
        return lax.ppermute(x, "samp", [(i, i ^ mask) for i in range(ranks)])

    def on_device(genotypes, counts, phenotypes):
        rows, samples = phenotypes.shape
        snps = genotypes.shape[1]
        scale = 1.0 / (snps * snp_ranks)
        width = snps // (CHUNKS * pieces)
        half = pieces // 2
        me = lax.axis_index("samp")
        root = jnp.sqrt(counts.astype(jnp.float32))
        narrow = jax.ShapeDtypeStruct((rows, half * width), jnp.bfloat16)
        wide = jax.ShapeDtypeStruct((rows, half * width), jnp.float32)
        held_shape = jax.ShapeDtypeStruct((samples, pieces * width), jnp.bfloat16)

        def load_pass(chunk, q):
            masks = halving[chunk % 2]
            own = sum(((me // m) % 2) << (levels - 1 - l) for l, m in enumerate(masks))
            place = jnp.stack([jnp.int32(chunk * pieces), own.astype(jnp.int32)])
            return pl.pallas_call(
                first_pass_kernel(pieces, width),
                out_shape=(narrow, wide, held_shape),
                in_specs=[smem(), vmem(), pl.BlockSpec(memory_space=pl.ANY)],
                out_specs=(vmem(), vmem(), vmem()),
                scratch_shapes=[pltpu.SemaphoreType.DMA((pieces,))],
                compiler_params=params(),
                name=f"load_pass_{chunk}",
            )(place, q, genotypes)

        def held_pass(q, held, chunk):
            return pl.pallas_call(
                pass_kernel(pieces, width),
                out_shape=(narrow, wide),
                in_specs=[vmem(), vmem()],
                out_specs=(vmem(), vmem()),
                compiler_params=params(),
                name=f"held_pass_{chunk}",
            )(q, held)

        def back_pass(parts, held, chunk):
            widths = [p.shape[1] for p in parts]
            return pl.pallas_call(
                back_kernel(widths, width),
                out_shape=(
                    jax.ShapeDtypeStruct((samples, rows), jnp.float32),
                    jax.ShapeDtypeStruct((rows, LANES), jnp.float32),
                ),
                in_specs=[vmem()] * (len(parts) + 1),
                out_specs=(vmem(), vmem()),
                compiler_params=params(),
                name=f"back_pass_{chunk}",
            )(*parts, held)

        def scatter(chunk, send, keep, norm):
            masks = halving[chunk % 2]
            for level, mask in enumerate(masks):
                size = keep.shape[1]
                if norm is not None:
                    send = jnp.concatenate([send, split3(norm)], axis=1)
                got = swap(send, mask)
                if norm is not None:
                    norm = norm + join3(got[:, size:])
                total = keep + got[:, :size].astype(jnp.float32)
                if level + 1 < levels:
                    keep = total[:, : size // 2]
                    send = total[:, size // 2 :].astype(jnp.bfloat16)
            for mask in full_masks:
                send = total.astype(jnp.bfloat16)
                if norm is not None:
                    send = jnp.concatenate([send, split3(norm)], axis=1)
                got = swap(send, mask)
                if norm is not None:
                    norm = norm + join3(got[:, width:])
                total = total + got[:, :width].astype(jnp.float32)
            return total, norm

        def gather(chunk, own):
            masks = halving[chunk % 2]
            first = swap(own, masks[2])
            pair = jnp.concatenate([own, first], axis=1)
            second = swap(pair, masks[1])
            third = swap(pair, masks[0])
            fourth = swap(second, masks[0])
            return [pair, second, third, fourth]

        def round_of(firsts, helds, norm, held_totals, norm_before):
            totals = []
            beta = None
            for chunk, (send, keep) in enumerate(firsts):
                total, summed = scatter(chunk, send, keep, norm if chunk == 0 else None)
                if chunk == 0:
                    norm_sum = summed
                    if held_totals is not None:
                        beta = norm_sum / norm_before
                if held_totals is not None:
                    total = total + beta[:, None] * held_totals[chunk]
                totals.append(total)
            backs = []
            for chunk, total in enumerate(totals):
                parts = gather(chunk, total.astype(jnp.bfloat16))
                backs.append(back_pass(parts, helds[chunk], chunk))
            back = sum(b[0] for b in backs).T
            square = jnp.sum(sum(b[1] for b in backs), axis=1)
            if snp_ranks > 1:
                back, square = lax.psum((back, square), "snp")
            return back, square, norm_sum, totals, beta

        q = (root[None, :] * phenotypes).astype(jnp.bfloat16)
        loaded = [load_pass(chunk, q) for chunk in range(CHUNKS)]
        helds = [l[2] for l in loaded]
        norm = jnp.sum(phenotypes * phenotypes, axis=1)
        back, square, norm0, totals, _ = round_of([l[:2] for l in loaded], helds, norm, None, None)
        alpha0 = norm0 / (square * scale + ridge * norm0)
        image = root[None, :] * back * scale + ridge * phenotypes
        residual = phenotypes - alpha0[:, None] * image

        q = (root[None, :] * residual).astype(jnp.bfloat16)
        firsts = [held_pass(q, helds[chunk], chunk) for chunk in range(CHUNKS)]
        norm = jnp.sum(residual * residual, axis=1)
        back, square, norm1, _, beta = round_of(firsts, helds, norm, totals, norm0)
        direction = residual + beta[:, None] * phenotypes
        alpha1 = norm1 / (square * scale + ridge * (norm1 + beta * beta * norm0))
        image = root[None, :] * back * scale + ridge * direction
        answer = alpha0[:, None] * phenotypes + alpha1[:, None] * direction
        return answer, residual - alpha1[:, None] * image

    placed = (P("samp", "snp"), P(("rep", "samp")), P(None, "samp"))
    return jax.shard_map(
        on_device,
        mesh=mesh,
        in_specs=placed,
        out_specs=(P(None, ("rep", "samp")), P(None, ("rep", "samp"))),
        check_vma=False,
    )
```

```python
import jax
import jax.numpy as jnp
from jax import lax
from jax.experimental import pallas as pl
from jax.experimental.pallas import tpu as pltpu
from jax.sharding import PartitionSpec as P

ridge = 1.0
CHUNKS = 2
LANES = 128


def first_pass_kernel(pieces, width):
    half = pieces // 2

    def body(place_ref, q_ref, g_ref, send_ref, keep_ref, held_ref, sems):
        def copy_of(p):
            at = pl.multiple_of(place_ref[p] * width, width)
            return pltpu.make_async_copy(
                g_ref.at[:, pl.ds(at, width)], held_ref.at[:, pl.ds(p * width, width)], sems.at[p]
            )

        order = list(range(half, pieces)) + list(range(half))
        for p in order:
            copy_of(p).start()
        q = q_ref[...]
        for p in order:
            copy_of(p).wait()
            sums = jnp.dot(q, held_ref[:, p * width : (p + 1) * width], preferred_element_type=jnp.float32)
            if p >= half:
                send_ref[:, (p - half) * width : (p - half + 1) * width] = sums.astype(jnp.bfloat16)
            else:
                keep_ref[:, p * width : (p + 1) * width] = sums

    return body


def pass_kernel(pieces, width):
    half = pieces // 2

    def body(q_ref, held_ref, send_ref, keep_ref):
        q = q_ref[...]
        for p in list(range(half, pieces)) + list(range(half)):
            sums = jnp.dot(q, held_ref[:, p * width : (p + 1) * width], preferred_element_type=jnp.float32)
            if p >= half:
                send_ref[:, (p - half) * width : (p - half + 1) * width] = sums.astype(jnp.bfloat16)
            else:
                keep_ref[:, p * width : (p + 1) * width] = sums

    return body


def back_kernel(widths, step):
    def body(*refs):
        part_refs = refs[: len(widths)]
        held_ref, back_ref, square_ref = refs[len(widths) :]
        back = jnp.zeros(back_ref.shape[::-1], jnp.float32)
        square = jnp.zeros(square_ref.shape, jnp.float32)
        base = 0
        for part_ref, width in zip(part_refs, widths):
            for at in range(0, width, step):
                t = part_ref[:, at : at + step]
                back = back + lax.dot_general(
                    held_ref[:, base + at : base + at + step],
                    t,
                    (((1,), (1,)), ((), ())),
                    preferred_element_type=jnp.float32,
                )
                wide = t.astype(jnp.float32)
                wide = wide * wide
                for lane in range(0, step, LANES):
                    square = square + wide[:, lane : lane + LANES]
            base += width
        back_ref[...] = back.T
        square_ref[...] = square

    return body


def vmem():
    return pl.BlockSpec(memory_space=pltpu.VMEM)


def smem():
    return pl.BlockSpec(memory_space=pltpu.SMEM)


def params():
    return pltpu.CompilerParams(vmem_limit_bytes=4 * 2**20)


def rounded(x):
    return lax.reduce_precision(x, 8, 7)


def parts_of(x):
    high = rounded(x)
    middle = rounded(x - high)
    low = rounded(x - high - middle)
    return [p.astype(jnp.bfloat16) for p in (high, middle, low)]


def joined(x):
    wide = x.astype(jnp.float32)
    return wide[:, :LANES] + wide[:, LANES : 2 * LANES] + wide[:, 2 * LANES :]


def folded(x):
    rows, length = x.shape
    tail = -length % LANES
    squares = jnp.pad(x * x, ((0, 0), (0, tail)))
    return jnp.sum(squares.reshape(rows, -1, LANES), axis=1)


def solution(mesh):
    ranks = mesh.shape["samp"]
    snp_ranks = mesh.shape["snp"]
    bits = ranks.bit_length() - 1
    assert ranks == 1 << bits and bits >= 4
    levels = 3
    pieces = 1 << levels
    full_masks = [1 << b for b in range(levels, bits)]

    def masks_of(chunk):
        orders = [[1, 2, 4], [1, 4, 2]]
        full = [full_masks, full_masks[::-1]]
        return [list(zip(a, b)) for a, b in (
            (orders[chunk % 2], orders[1 - chunk % 2]), (full[chunk % 2], full[1 - chunk % 2]))]

    def swap(x, masks):
        return lax.ppermute(x, "samp", [(i, i ^ masks[i % 2]) for i in range(ranks)])

    def piece_table(chunk):
        me = lax.axis_index("samp")
        own = ((me & 1) << 2) | (me & 2) | ((me >> 2) & 1)
        plain = [p for p in range(pieces)]
        turned = [(p & 4) | ((p & 1) << 1) | ((p >> 1) & 1) for p in range(pieces)]
        even = jnp.array(plain[:4] + turned[4:], jnp.int32)
        odd = jnp.array(turned[:4] + plain[4:], jnp.int32)
        if chunk % 2:
            even, odd = odd, even
        return chunk * pieces + (own.astype(jnp.int32) ^ jnp.where(me & 1 == 0, even, odd))

    def on_device(genotypes, counts, phenotypes):
        rows, samples = phenotypes.shape
        snps = genotypes.shape[1]
        scale = 1.0 / (snps * snp_ranks)
        width = snps // (CHUNKS * pieces)
        half = pieces // 2
        genotypes = pltpu.with_memory_space_constraint(genotypes, pltpu.HBM)
        root = jnp.sqrt(counts.astype(jnp.float32))
        narrow = jax.ShapeDtypeStruct((rows, half * width), jnp.bfloat16)
        wide = jax.ShapeDtypeStruct((rows, half * width), jnp.float32)
        held_shape = pltpu.VMEM((samples, pieces * width), jnp.bfloat16)

        def load_pass(chunk, q):
            return pl.pallas_call(
                first_pass_kernel(pieces, width),
                out_shape=(narrow, wide, held_shape),
                in_specs=[smem(), vmem(), pl.BlockSpec(memory_space=pltpu.HBM)],
                out_specs=(vmem(), vmem(), vmem()),
                scratch_shapes=[pltpu.SemaphoreType.DMA((pieces,))],
                compiler_params=params(),
                name=f"load_pass_{chunk}",
            )(piece_table(chunk), q, genotypes)

        def held_pass(q, held, chunk):
            return pl.pallas_call(
                pass_kernel(pieces, width),
                out_shape=(narrow, wide),
                in_specs=[vmem(), vmem()],
                out_specs=(vmem(), vmem()),
                compiler_params=params(),
                name=f"held_pass_{chunk}",
            )(q, held)

        def back_pass(parts, held, chunk):
            widths = [p.shape[1] for p in parts]
            return pl.pallas_call(
                back_kernel(widths, width),
                out_shape=(
                    jax.ShapeDtypeStruct((rows, samples), jnp.float32),
                    jax.ShapeDtypeStruct((rows, LANES), jnp.float32),
                ),
                in_specs=[vmem()] * (len(parts) + 1),
                out_specs=(vmem(), vmem()),
                compiler_params=params(),
                name=f"back_pass_{chunk}",
            )(*parts, held)

        def scatter(chunk, send, keep, norm):
            masks, wide_masks = masks_of(chunk)
            for level, mask in enumerate(masks):
                size = keep.shape[1]
                if norm is not None:
                    send = jnp.concatenate([send, *parts_of(norm)], axis=1)
                got = swap(send, mask)
                if norm is not None:
                    norm = norm + joined(got[:, size:])
                total = keep + got[:, :size].astype(jnp.float32)
                if level + 1 < levels:
                    keep = total[:, : size // 2]
                    send = total[:, size // 2 :].astype(jnp.bfloat16)
            for mask in wide_masks:
                send = total.astype(jnp.bfloat16)
                if norm is not None:
                    send = jnp.concatenate([send, *parts_of(norm)], axis=1)
                got = swap(send, mask)
                if norm is not None:
                    norm = norm + joined(got[:, width:])
                total = total + got[:, :width].astype(jnp.float32)
            return total, norm

        def gather(chunk, own):
            masks, _ = masks_of(chunk)
            first = swap(own, masks[2])
            pair = jnp.concatenate([own, first], axis=1)
            second = swap(pair, masks[1])
            third = swap(pair, masks[0])
            fourth = swap(second, masks[0])
            return [pair, second, third, fourth]

        def round_of(firsts, helds, norm, held_totals, norm_before):
            totals = []
            beta = None
            for chunk, (send, keep) in enumerate(firsts):
                total, summed = scatter(chunk, send, keep, norm if chunk == 0 else None)
                if chunk == 0:
                    norm_sum = jnp.sum(summed, axis=1)
                    if held_totals is not None:
                        beta = norm_sum / norm_before
                if held_totals is not None:
                    total = total + beta[:, None] * held_totals[chunk]
                totals.append(total)
            backs = []
            for chunk, total in enumerate(totals):
                parts = gather(chunk, total.astype(jnp.bfloat16))
                backs.append(back_pass(parts, helds[chunk], chunk))
            back = sum(b[0] for b in backs)
            square = jnp.sum(sum(b[1] for b in backs), axis=1)
            if snp_ranks > 1:
                back, square = lax.psum((back, square), "snp")
            return back, square, norm_sum, totals, beta

        q = (root[None, :] * phenotypes).astype(jnp.bfloat16)
        loaded = [load_pass(chunk, q) for chunk in range(CHUNKS)]
        helds = [pltpu.with_memory_space_constraint(l[2], pltpu.VMEM) for l in loaded]
        norm = folded(phenotypes)
        back, square, norm0, totals, _ = round_of([l[:2] for l in loaded], helds, norm, None, None)
        alpha0 = norm0 / (square * scale + ridge * norm0)
        image = root[None, :] * back * scale + ridge * phenotypes
        residual = phenotypes - alpha0[:, None] * image

        q = (root[None, :] * residual).astype(jnp.bfloat16)
        firsts = [held_pass(q, helds[chunk], chunk) for chunk in range(CHUNKS)]
        norm = folded(residual)
        back, square, norm1, _, beta = round_of(firsts, helds, norm, totals, norm0)
        direction = residual + beta[:, None] * phenotypes
        alpha1 = norm1 / (square * scale + ridge * (norm1 + beta * beta * norm0))
        image = root[None, :] * back * scale + ridge * direction
        answer = alpha0[:, None] * phenotypes + alpha1[:, None] * direction
        return answer, residual - alpha1[:, None] * image

    placed = (P("samp", "snp"), P(("rep", "samp")), P(None, "samp"))
    return jax.shard_map(
        on_device,
        mesh=mesh,
        in_specs=placed,
        out_specs=(P(None, ("rep", "samp")), P(None, ("rep", "samp"))),
        check_vma=False,
    )
```

```python
import jax
import jax.numpy as jnp
from jax import lax
from jax.experimental import pallas as pl
from jax.experimental.pallas import tpu as pltpu
from jax.sharding import PartitionSpec as P

ridge = 1.0
LANES = 128
LEVELS = 3
UNITS = 16
COST = 512
FLIP = True
SAME = True


def vmem():
    return pl.BlockSpec(memory_space=pltpu.VMEM)


def hbm():
    return pl.BlockSpec(memory_space=pltpu.HBM)


def params(megabytes=4):
    return pltpu.CompilerParams(vmem_limit_bytes=megabytes * 2**20)


def load_kernel(upper, unit, dims):
    levels = len(dims)

    def body(*refs):
        if upper:
            counts_ref, given_ref, g_ref, sums_ref, held_ref, root_ref, q_ref, norm_ref = refs[:8]
            count_here, given_here, sems, small_sems = refs[8:]
            small = [pltpu.make_async_copy(counts_ref, count_here, small_sems.at[0]),
                     pltpu.make_async_copy(given_ref, given_here, small_sems.at[1])]
            for copy in small:
                copy.start()
        else:
            q_ref, g_ref, sums_ref, held_ref, sems = refs
        me = lax.axis_index("samp")
        half = held_ref.shape[1]
        piece = half >> levels
        owner = (me ^ upper) & 1
        copies = []
        for p in range(1 << levels):
            column = owner << levels
            for level, (even, odd) in enumerate(dims):
                turn = levels - 1 - level
                flip = jnp.where((me & jnp.where(owner == 0, even, odd)) == 0, 0, 1)
                column = column | ((flip ^ ((p >> turn) & 1)) << turn)
            for at in range(0, piece, unit):
                start = pl.multiple_of(column * piece + at, unit)
                place = p * piece + at
                copies.append((place, pltpu.make_async_copy(
                    g_ref.at[:, pl.ds(start, unit)], held_ref.at[:, place : place + unit], sems.at[len(copies)])))
        for _, copy in copies:
            copy.start()
        if upper:
            for copy in small:
                copy.wait()
            given = given_here[...]
            root = jnp.sqrt(count_here[...].astype(jnp.float32))
            root_ref[...] = root
            q_ref[...] = (root * given).astype(jnp.bfloat16)
            total = jnp.sum(given * given, axis=1, keepdims=True)
            lane = lax.broadcasted_iota(jnp.int32, norm_ref.shape, 1)
            norm_ref[...] = jnp.where(lane == 0, total, 0.0)
        q = q_ref[...]
        for place, copy in copies:
            copy.wait()
            sums = jnp.dot(q, held_ref[:, place : place + unit], preferred_element_type=jnp.float32)
            sums_ref[:, place : place + unit] = sums.astype(sums_ref.dtype)

    return body


def held_kernel(unit):
    def body(q_ref, held_ref, sums_ref):
        q = q_ref[...]
        for at in range(0, held_ref.shape[1], unit):
            sums = jnp.dot(q, held_ref[:, at : at + unit], preferred_element_type=jnp.float32)
            sums_ref[:, at : at + unit] = sums.astype(sums_ref.dtype)

    return body


def back_kernel(base, width):
    tile = 2 * LANES

    def body(part_ref, held_ref, back_ref, square_ref):
        tall = jnp.zeros(back_ref.shape[::-1], jnp.float32)
        flat = jnp.zeros(back_ref.shape, jnp.float32)
        square = jnp.zeros(square_ref.shape, jnp.float32)
        for turn, at in enumerate(range(0, width, tile)):
            t = part_ref[:, at : at + tile]
            g = held_ref[:, base + at : base + at + tile]
            over = (((1,), (1,)), ((), ()))
            if turn % 3 < 2:
                tall = tall + lax.dot_general(g, t, over, preferred_element_type=jnp.float32)
            else:
                flat = flat + lax.dot_general(t, g, over, preferred_element_type=jnp.float32)
            wide = t.astype(jnp.float32)
            wide = wide * wide
            for lane in range(0, tile, LANES):
                square = square + wide[:, lane : lane + LANES]
        back_ref[...] = tall.T + flat
        square_ref[...] = square

    return body


def rounded(x):
    return lax.reduce_precision(x, 8, 7)


def parts_of(x):
    high = rounded(x)
    middle = rounded(x - high)
    low = rounded(x - high - middle)
    return [p.astype(jnp.bfloat16) for p in (high, middle, low)]


def joined(x):
    wide = x.astype(jnp.float32)
    return wide[:, :LANES] + wide[:, LANES : 2 * LANES] + wide[:, 2 * LANES :]


def solution(mesh):
    ranks = mesh.shape["samp"]
    snp_ranks = mesh.shape["snp"]
    bits = ranks.bit_length() - 1
    assert ranks == 1 << bits and bits >= 3

    far = [1 << b for b in range(3, bits)]
    if FLIP:
        far = far[:-1] + [sum(far[-2:])]
    dims = [(1, 1)] + list(zip([4, 2] + (far if SAME else far[::-1]), [2, 4] + far))

    def swap(x, dims):
        return lax.ppermute(x, "samp", [(i, i ^ dims[i % 2]) for i in range(ranks)])

    def on_device(genotypes, counts, phenotypes):
        rows, samples = phenotypes.shape
        snps = genotypes.shape[1]
        scale = 1.0 / (snps * snp_ranks)
        unit = snps // UNITS
        half = snps // 2
        step = min(unit, half >> (LEVELS - 1))

        def cost(columns, weight):
            return pl.CostEstimate(flops=weight * columns * samples, bytes_accessed=0, transcendentals=0)

        def load_pass(upper, *args):
            more, scratch, small_sems = (), [], []
            if upper:
                more = (
                    jax.ShapeDtypeStruct((1, samples), jnp.float32),
                    jax.ShapeDtypeStruct((rows, samples), jnp.bfloat16),
                    jax.ShapeDtypeStruct((rows, LANES), jnp.float32),
                )
                scratch = [pltpu.VMEM((1, samples), jnp.int32), pltpu.VMEM((rows, samples), jnp.float32)]
                small_sems = [pltpu.SemaphoreType.DMA((2,))]
            return pl.pallas_call(
                load_kernel(upper, step, dims[1:LEVELS]),
                out_shape=(
                    jax.ShapeDtypeStruct((rows, half), jnp.bfloat16 if upper else jnp.float32),
                    pltpu.VMEM((samples, half), jnp.bfloat16),
                ) + more,
                in_specs=[hbm() if upper else vmem()] * len(args) + [hbm()],
                out_specs=(vmem(),) * (2 + len(more)),
                scratch_shapes=scratch + [pltpu.SemaphoreType.DMA((half // step,))] + small_sems,
                compiler_params=params(24),
                cost_estimate=cost(half, COST),
                name=f"load_pass_{upper}",
            )(*args, genotypes)

        def held_pass(upper, q, held):
            return pl.pallas_call(
                held_kernel(unit),
                out_shape=jax.ShapeDtypeStruct((rows, half), jnp.bfloat16 if upper else jnp.float32),
                in_specs=[vmem(), vmem()],
                out_specs=vmem(),
                compiler_params=params(),
                cost_estimate=cost(half, COST // 2),
                name=f"held_pass_{upper}",
            )(q, held)

        def back_pass(part, held, base):
            return pl.pallas_call(
                back_kernel(base, part.shape[1]),
                out_shape=(
                    jax.ShapeDtypeStruct((rows, samples), jnp.float32),
                    jax.ShapeDtypeStruct((rows, LANES), jnp.float32),
                ),
                in_specs=[vmem(), vmem()],
                out_specs=(vmem(), vmem()),
                compiler_params=params(),
                cost_estimate=cost(part.shape[1], COST),
                name=f"back_pass_{base}",
            )(part, held)

        def reduce(send, total, norm):
            for level, dim in enumerate(dims):
                if level >= LEVELS:
                    send = total.astype(jnp.bfloat16)
                elif level:
                    middle = total.shape[1] // 2
                    send, total = total[:, middle:].astype(jnp.bfloat16), total[:, :middle]
                width = total.shape[1]
                got = swap(jnp.concatenate([send, *parts_of(norm)], axis=1), dim)
                norm = norm + joined(got[:, width:])
                total = total + got[:, :width].astype(jnp.float32)
            return total, norm

        def spread(own, held_lower, held_upper):
            backs = [back_pass(own, held_lower, 0)]
            whole = own
            for level in range(LEVELS - 1, 0, -1):
                width = whole.shape[1]
                got = swap(whole, dims[level])
                if level == 1:
                    across = swap(whole, dims[0])
                    backs.append(back_pass(across, held_upper, 0))
                    got, backs = lax.optimization_barrier((got, backs))
                backs.append(back_pass(got, held_lower, width))
                if level > 1:
                    whole = jnp.concatenate([whole, got], axis=1)
            across = swap(got, dims[0])
            backs.append(back_pass(across, held_upper, width))
            return backs

        def round_of(send, keep, helds, norm, before, norm_before):
            total, norm = reduce(send, keep, norm)
            norm_sum = jnp.sum(norm, axis=1)
            if before is not None:
                total = total + (norm_sum / norm_before)[:, None] * before
            backs = spread(total.astype(jnp.bfloat16), *helds)
            back = sum(b[0] for b in backs)
            square = jnp.sum(sum(b[1] for b in backs), axis=1)
            if snp_ranks > 1:
                back, square = lax.psum((back, square), "snp")
            return back, square, norm_sum, total

        small = [pltpu.with_memory_space_constraint(x, pltpu.HBM) for x in (counts.reshape(1, samples), phenotypes)]
        send, upper, root, q, norm = load_pass(1, *small)
        keep, lower = load_pass(0, q)
        helds = [pltpu.with_memory_space_constraint(h, pltpu.VMEM) for h in (lower, upper)]
        back, square, norm0, total = round_of(send, keep, helds, norm, None, None)
        alpha0 = norm0 / (square * scale + ridge * norm0)
        image = root * back * scale + ridge * phenotypes
        residual = phenotypes - alpha0[:, None] * image

        q = (root * residual).astype(jnp.bfloat16)
        send = held_pass(1, q, helds[1])
        keep = held_pass(0, q, helds[0])
        tail = -samples % LANES
        squares = jnp.pad(residual * residual, ((0, 0), (0, tail)))
        norm = jnp.sum(squares.reshape(rows, -1, LANES), axis=1)
        back, square, norm1, _ = round_of(send, keep, helds, norm, total, norm0)
        beta = norm1 / norm0
        direction = residual + beta[:, None] * phenotypes
        alpha1 = norm1 / (square * scale + ridge * (norm1 + beta * beta * norm0))
        image = root * back * scale + ridge * direction
        answer = alpha0[:, None] * phenotypes + alpha1[:, None] * direction
        return answer, residual - alpha1[:, None] * image

    placed = (P("samp", "snp"), P(("rep", "samp")), P(None, "samp"))
    return jax.shard_map(
        on_device,
        mesh=mesh,
        in_specs=placed,
        out_specs=(P(None, ("rep", "samp")), P(None, ("rep", "samp"))),
        check_vma=False,
    )
```

```python
import jax
import jax.numpy as jnp
from jax import lax
from jax.experimental import pallas as pl
from jax.experimental.pallas import tpu as pltpu
from jax.sharding import PartitionSpec as P

ridge = 1.0
LANES = 128
LEVELS = 3
UNITS = 8
COST = 2048
EARLY = 2
FLIP = True
SAME = True


def vmem():
    return pl.BlockSpec(memory_space=pltpu.VMEM)


def hbm():
    return pl.BlockSpec(memory_space=pltpu.HBM)


def params(megabytes=4):
    return pltpu.CompilerParams(vmem_limit_bytes=megabytes * 2**20)


def load_kernel(upper, chosen, piece, unit, dims):
    levels = len(dims)

    def body(*refs):
        if upper:
            counts_ref, given_ref, g_ref, sums_ref, held_ref, root_ref, q_ref, norm_ref = refs[:8]
            count_here, given_here, sems, small_sems = refs[8:]
            small = [pltpu.make_async_copy(counts_ref, count_here, small_sems.at[0]),
                     pltpu.make_async_copy(given_ref, given_here, small_sems.at[1])]
            for copy in small:
                copy.start()
        else:
            q_ref, g_ref, sums_ref, held_ref, sems = refs
        me = lax.axis_index("samp")
        owner = (me ^ upper) & 1
        copies = []
        for turn_at, p in enumerate(chosen):
            column = owner << levels
            for level, (even, odd) in enumerate(dims):
                turn = levels - 1 - level
                flip = jnp.where((me & jnp.where(owner == 0, even, odd)) == 0, 0, 1)
                column = column | ((flip ^ ((p >> turn) & 1)) << turn)
            for at in range(0, piece, unit):
                start = pl.multiple_of(column * piece + at, unit)
                place = turn_at * piece + at
                copies.append((place, pltpu.make_async_copy(
                    g_ref.at[:, pl.ds(start, unit)], held_ref.at[:, place : place + unit], sems.at[len(copies)])))
        for _, copy in copies:
            copy.start()
        if upper:
            for copy in small:
                copy.wait()
            given = given_here[...]
            root = jnp.sqrt(count_here[...].astype(jnp.float32))
            root_ref[...] = root
            q_ref[...] = (root * given).astype(jnp.bfloat16)
            total = jnp.sum(given * given, axis=1, keepdims=True)
            lane = lax.broadcasted_iota(jnp.int32, norm_ref.shape, 1)
            norm_ref[...] = jnp.where(lane == 0, total, 0.0)
        q = q_ref[...]
        for place, copy in copies:
            copy.wait()
            sums = jnp.dot(q, held_ref[:, place : place + unit], preferred_element_type=jnp.float32)
            sums_ref[:, place : place + unit] = sums.astype(sums_ref.dtype)

    return body


def held_kernel(unit):
    def body(q_ref, held_ref, sums_ref):
        q = q_ref[...]
        for at in range(0, held_ref.shape[1], unit):
            sums = jnp.dot(q, held_ref[:, at : at + unit], preferred_element_type=jnp.float32)
            sums_ref[:, at : at + unit] = sums.astype(sums_ref.dtype)

    return body


def back_kernel(base, width):
    tile = 2 * LANES

    def body(part_ref, held_ref, back_ref, square_ref):
        tall = jnp.zeros(back_ref.shape[::-1], jnp.float32)
        flat = jnp.zeros(back_ref.shape, jnp.float32)
        square = jnp.zeros(square_ref.shape, jnp.float32)
        for turn, at in enumerate(range(0, width, tile)):
            t = part_ref[:, at : at + tile]
            g = held_ref[:, base + at : base + at + tile]
            over = (((1,), (1,)), ((), ()))
            if turn % 3 < 2:
                tall = tall + lax.dot_general(g, t, over, preferred_element_type=jnp.float32)
            else:
                flat = flat + lax.dot_general(t, g, over, preferred_element_type=jnp.float32)
            wide = t.astype(jnp.float32)
            wide = wide * wide
            for lane in range(0, tile, LANES):
                square = square + wide[:, lane : lane + LANES]
        back_ref[...] = tall.T + flat
        square_ref[...] = square

    return body


def rounded(x):
    return lax.reduce_precision(x, 8, 7)


def parts_of(x):
    high = rounded(x)
    middle = rounded(x - high)
    low = rounded(x - high - middle)
    return [p.astype(jnp.bfloat16) for p in (high, middle, low)]


def joined(x):
    wide = x.astype(jnp.float32)
    return wide[:, :LANES] + wide[:, LANES : 2 * LANES] + wide[:, 2 * LANES :]


def solution(mesh):
    ranks = mesh.shape["samp"]
    snp_ranks = mesh.shape["snp"]
    bits = ranks.bit_length() - 1
    assert ranks == 1 << bits and bits >= 3

    far = [1 << b for b in range(3, bits)]
    if FLIP:
        far = far[:-1] + [sum(far[-2:])]
    dims = [(1, 1)] + list(zip([4, 2] + (far if SAME else far[::-1]), [2, 4] + far))

    def swap(x, dims):
        return lax.ppermute(x, "samp", [(i, i ^ dims[i % 2]) for i in range(ranks)])

    def on_device(genotypes, counts, phenotypes):
        rows, samples = phenotypes.shape
        snps = genotypes.shape[1]
        scale = 1.0 / (snps * snp_ranks)
        unit = snps // UNITS
        half = snps // 2
        step = min(unit, half >> (LEVELS - 1))

        def cost(columns, weight):
            return pl.CostEstimate(flops=weight * columns * samples, bytes_accessed=0, transcendentals=0)

        pieces = 1 << (LEVELS - 1)
        piece = half // pieces
        groups = ((0, range(pieces // 2)), (0, range(pieces // 2, pieces)), (1, range(pieces)))

        def sums_of(group):
            upper, chosen = groups[group]
            return jax.ShapeDtypeStruct((rows, len(chosen) * piece), jnp.bfloat16 if upper else jnp.float32)

        def load_pass(group, *args):
            upper, chosen = groups[group]
            size = len(chosen) * piece
            more, scratch, small_sems = (), [], []
            if upper:
                more = (
                    jax.ShapeDtypeStruct((1, samples), jnp.float32),
                    jax.ShapeDtypeStruct((rows, samples), jnp.bfloat16),
                    jax.ShapeDtypeStruct((rows, LANES), jnp.float32),
                )
                scratch = [pltpu.VMEM((1, samples), jnp.int32), pltpu.VMEM((rows, samples), jnp.float32)]
                small_sems = [pltpu.SemaphoreType.DMA((2,))]
            return pl.pallas_call(
                load_kernel(upper, tuple(chosen), piece, step, dims[1:LEVELS]),
                out_shape=(sums_of(group), pltpu.VMEM((samples, size), jnp.bfloat16)) + more,
                in_specs=[hbm() if upper else vmem()] * len(args) + [hbm()],
                out_specs=(vmem(),) * (2 + len(more)),
                scratch_shapes=scratch + [pltpu.SemaphoreType.DMA((size // step,))] + small_sems,
                compiler_params=params(24),
                cost_estimate=cost(size, COST),
                name=f"load_pass_{group}",
            )(*args, genotypes)

        def held_pass(group, q, held):
            return pl.pallas_call(
                held_kernel(step),
                out_shape=sums_of(group),
                in_specs=[vmem(), vmem()],
                out_specs=vmem(),
                compiler_params=params(),
                cost_estimate=cost(held.shape[1], COST // 2),
                name=f"held_pass_{group}",
            )(q, held)

        def back_pass(part, held, base):
            return pl.pallas_call(
                back_kernel(base, part.shape[1]),
                out_shape=(
                    jax.ShapeDtypeStruct((rows, samples), jnp.float32),
                    jax.ShapeDtypeStruct((rows, LANES), jnp.float32),
                ),
                in_specs=[vmem(), vmem()],
                out_specs=(vmem(), vmem()),
                compiler_params=params(),
                cost_estimate=cost(part.shape[1], COST),
                name=f"back_pass_{base}",
            )(part, held)

        def reduce(stay, leave, send, norm):
            for level, dim in enumerate(dims):
                if level == 1:
                    middle = stay.shape[1]
                    send = (leave + got[:, middle : 2 * middle].astype(jnp.float32)).astype(jnp.bfloat16)
                    total = stay + got[:, :middle].astype(jnp.float32)
                elif level >= LEVELS:
                    send = total.astype(jnp.bfloat16)
                elif level:
                    middle = total.shape[1] // 2
                    send, total = total[:, middle:].astype(jnp.bfloat16), total[:, :middle]
                width = send.shape[1]
                got = swap(jnp.concatenate([send, *parts_of(norm)], axis=1), dim)
                norm = norm + joined(got[:, width:])
                if level:
                    total = total + got[:, :width].astype(jnp.float32)
            return total, norm

        def spread(own, held_stay, held_leave, held_upper):
            width = own.shape[1]
            parts = [own]
            for level in range(LEVELS - 1, 0, -1):
                parts = parts + [swap(p, dims[level]) for p in parts]
            last = parts.pop()
            across = [swap(p, dims[0]) for p in parts]
            kept = len(parts) + 1 >> 1
            backs = [
                back_pass(p, held_leave if n >= kept else held_stay, n % kept * width) for n, p in enumerate(parts)
            ]
            backs += [back_pass(p, held_upper, n * width) for n, p in enumerate(across[:EARLY])]
            last, backs = lax.optimization_barrier((last, backs))
            backs += [back_pass(p, held_upper, (EARLY + n) * width) for n, p in enumerate(across[EARLY:])]
            backs.append(back_pass(last, held_leave, len(parts) % kept * width))
            backs.append(back_pass(swap(last, dims[0]), held_upper, len(parts) * width))
            return backs

        def round_of(sums, helds, norm, before, norm_before):
            total, norm = reduce(*sums, norm)
            norm_sum = jnp.sum(norm, axis=1)
            if before is not None:
                total = total + (norm_sum / norm_before)[:, None] * before
            backs = spread(total.astype(jnp.bfloat16), *helds)
            back = sum(b[0] for b in backs)
            square = jnp.sum(sum(b[1] for b in backs), axis=1)
            if snp_ranks > 1:
                back, square = lax.psum((back, square), "snp")
            return back, square, norm_sum, total

        small = [pltpu.with_memory_space_constraint(x, pltpu.HBM) for x in (counts.reshape(1, samples), phenotypes)]
        send, upper, root, q, norm = load_pass(2, *small)
        leave, leaving = load_pass(1, q)
        stay, staying = load_pass(0, q)
        helds = [pltpu.with_memory_space_constraint(h, pltpu.VMEM) for h in (staying, leaving, upper)]
        back, square, norm0, total = round_of((stay, leave, send), helds, norm, None, None)
        alpha0 = norm0 / (square * scale + ridge * norm0)
        image = root * back * scale + ridge * phenotypes
        residual = phenotypes - alpha0[:, None] * image

        q = (root * residual).astype(jnp.bfloat16)
        sums = [held_pass(group, q, helds[group]) for group in (2, 1, 0)][::-1]
        tail = -samples % LANES
        squares = jnp.pad(residual * residual, ((0, 0), (0, tail)))
        norm = jnp.sum(squares.reshape(rows, -1, LANES), axis=1)
        back, square, norm1, _ = round_of(sums, helds, norm, total, norm0)
        beta = norm1 / norm0
        direction = residual + beta[:, None] * phenotypes
        alpha1 = norm1 / (square * scale + ridge * (norm1 + beta * beta * norm0))
        image = root * back * scale + ridge * direction
        answer = alpha0[:, None] * phenotypes + alpha1[:, None] * direction
        return answer, residual - alpha1[:, None] * image

    placed = (P("samp", "snp"), P(("rep", "samp")), P(None, "samp"))
    return jax.shard_map(
        on_device,
        mesh=mesh,
        in_specs=placed,
        out_specs=(P(None, ("rep", "samp")), P(None, ("rep", "samp"))),
        check_vma=False,
    )
```
